32 devices in a mesh: frame: 8 (over z, core), head: 4 (over y, x).
Axes of the slice: x: 2, y: 2, z: 4, core: 2. Of those that a mesh axis runs over, the one named last changes fastest.
Arguments:
- queries: bfloat16 [512, 8192], P('frame', 'head'), may hold values from -6 to 6
- q_gain: float32 [128], replicated, may hold values from 0.1 to 1.9
- keys: bfloat16 [12800, 1024], P('frame', 'head'), may hold values from -6 to 6
- k_gain: float32 [128], replicated, may hold values from 0.1 to 1.9
- values: bfloat16 [12800, 1024], P('frame', 'head'), may hold values from -6 to 6
- out_grad: bfloat16 [512, 8192], P('frame', 'head'), may hold values from -384 to 384
- w_query: bfloat16 [8192, 8192], P(None, 'head'), may hold values from -0.0625 to 0.0625
- span_mask: int32 [32, 8], P(None, 'frame'), may hold values from 0 to 1, as said below
- frame_len: int32 [8], P('frame'), may hold values from 400 to 1600
Outputs:
- text_grad: float32 [512, 8192], P('frame', 'head')
- key_grad: float32 [12800, 1024], P('frame', 'head')
- value_grad: float32 [12800, 1024], P('frame', 'head')
The draws below stay inside these ranges and needn't reach their ends.
Inputs may be any that keep to these rules, and one draw needn't show every extreme that they name: `span_mask`: every text span sees at least one frame.
All inputs are finite; a program needn't handle non-finite values.
Results may differ from the reference program's by a relative error of at most 0.012.
The reference program's roundings to bfloat16 on the way (of `qb`, `kb` and `dq`) count: a program that leaves them out, or rounds other values in their place, can miss the bound.
Values may be sent and summed in bfloat16 or wider, within the bound.
No kernel may reach another device: no remote copies, remote signals or barrier semaphores. Data moves between devices by JAX's collectives and lax.ppermute only.
A program may use at most 192 MiB of HBM per device.

```python
import jax
import jax.numpy as jnp
from jax import lax

D = 8192
QH = 64
KVH = 8
HD = 128
KF = 1600
BLK = 16
TXT = 512
FRAMES = 8
KEYS = 12800
SPANS = 32


def draw_span_mask(key, part):
    key_level, key_bits, key_pick = jax.random.split(key, 3)
    level = jax.random.randint(key_level, (1, FRAMES), 1, 5)
    bits = jax.random.randint(key_bits, (SPANS, FRAMES), 0, 4) < level
    pick = jax.random.randint(key_pick, (SPANS, 1), 0, FRAMES)
    chosen = pick == jnp.arange(FRAMES, dtype=jnp.int32)[None, :]
    return (bits | chosen).astype(jnp.int32)


def touch_ends(array, key, least, high):
    longest = array.shape.index(max(array.shape))
    spots = []
    for shift in (0, 1):
        where = [jax.random.randint(jax.random.fold_in(key, axis), (), 0, length) for axis, length in enumerate(array.shape)]
        where[longest] = (where[longest] + shift) % array.shape[longest]
        spots.append(tuple(where))
    return array.at[spots[0]].set(least).at[spots[1]].set(high)


def steps_of(key, extent, cuts, least, largest):
    level, own = 1.0, jax.random.fold_in(key, 6)
    for position, blocks in cuts:
        heights = jnp.exp(jax.random.uniform(jax.random.fold_in(own, position), (blocks,), jnp.float32, least / len(cuts), largest / len(cuts)))
        level = level * jnp.repeat(heights, extent[position] // blocks).reshape([-1 if axis == position else 1 for axis in range(len(extent))])
    return level


def normal_values(stream_key, dims, width, reach, pieces=(), kind=jnp.bfloat16):
    entries = jax.random.normal(stream_key, dims, jnp.float32) * width
    if len(pieces) > 0:
        entries = steps_of(stream_key, dims, pieces, -0.22, 0.18) * entries
    return jnp.clip(entries, min=-reach, max=reach).astype(kind)


def setup_inputs(seed: int = 0) -> dict:
    streams_of = jax.random.split(jax.random.key(seed), 10)
    queries = normal_values(streams_of[0], (TXT, QH * HD), 1.0, 6.0, ((0, 8), (1, 4)))
    q_gain = jnp.clip(1.0 + 0.18 * jax.random.normal(streams_of[1], (HD,), jnp.float32), 0.1, 1.9)
    keys = normal_values(streams_of[2], (KEYS, KVH * HD), 1.0, 6.0, ((0, 8), (1, 4)))
    k_gain = jnp.clip(1.0 + 0.18 * jax.random.normal(streams_of[3], (HD,), jnp.float32), 0.1, 1.9)
    values = normal_values(streams_of[4], (KEYS, KVH * HD), 1.0, 6.0, ((0, 8), (1, 4)))
    out_grad = normal_values(streams_of[5], (TXT, QH * HD), 64.0, 384.0, ((0, 8), (1, 4)))
    w_query = normal_values(streams_of[6], (D, QH * HD), D ** -0.5, 0.0625, ((1, 4),))
    span_mask = draw_span_mask(jax.random.fold_in(streams_of[9], 71), 0)
    frame_len = touch_ends(jax.random.randint(streams_of[8], (FRAMES,), KF // 4, KF + 1), jax.random.fold_in(streams_of[8], 1), KF // 4, KF).astype(jnp.int32)
    return {"queries": queries, "q_gain": q_gain, "keys": keys, "k_gain": k_gain, "values": values, "out_grad": out_grad, "w_query": w_query, "span_mask": span_mask, "frame_len": frame_len}


EPS = 1e-05

def reference(queries, q_gain, keys, k_gain, values, out_grad, w_query, span_mask, frame_len):
    group = QH // KVH
    q = queries.astype(jnp.float32).reshape(TXT, QH, HD)
    rq = lax.rsqrt(lax.optimization_barrier(jnp.mean(q * q, axis=-1, keepdims=True)) + EPS)
    qb = (q * rq * q_gain * HD ** (-0.5)).astype(jnp.bfloat16)
    k = keys.astype(jnp.float32).reshape(KEYS, KVH, HD)
    rk = lax.rsqrt(lax.optimization_barrier(jnp.mean(k * k, axis=-1, keepdims=True)) + EPS)
    kb = (k * rk * k_gain).astype(jnp.bfloat16)
    key_pos = jnp.arange(KEYS)
    frame_of = key_pos // KF
    key_ok = key_pos % KF < frame_len[frame_of]
    span_of = jnp.arange(TXT) // BLK
    visible = (span_mask[span_of][:, frame_of] > 0) & key_ok[None, :]
    q_groups = qb.reshape(TXT, KVH, group, HD).transpose(1, 2, 0, 3)
    d_groups = out_grad.reshape(TXT, KVH, group, HD).transpose(1, 2, 0, 3)
    k_groups = kb.transpose(1, 0, 2)
    v_groups = values.reshape(KEYS, KVH, HD).transpose(1, 0, 2)

    def per_kv(items):
        q_heads, d_heads, k_head, v_head = items

        def per_head(carry, pair):
            dk_acc, dv_acc = carry
            q_one, d_one = pair
            scores = jnp.dot(q_one, k_head.T, preferred_element_type=jnp.float32)
            expd = jnp.where(visible, jnp.exp(scores), jnp.float32(0.0))
            dprob = jnp.dot(d_one, v_head.T, preferred_element_type=jnp.float32)
            total = lax.optimization_barrier(jnp.sum(expd, axis=1))
            weighted = lax.optimization_barrier(jnp.sum(expd * dprob, axis=1))
            prob = expd / total[:, None]
            dscore = prob * (dprob - (weighted / total)[:, None])
            prob_b = prob.astype(jnp.bfloat16)
            dscore_b = dscore.astype(jnp.bfloat16)
            dv_acc = dv_acc + jnp.dot(prob_b.T, d_one, preferred_element_type=jnp.float32)
            dk_acc = dk_acc + jnp.dot(dscore_b.T, q_one, preferred_element_type=jnp.float32)
            dq_one = jnp.dot(dscore_b, k_head, preferred_element_type=jnp.float32)
            return ((dk_acc, dv_acc), dq_one)
        start = (jnp.zeros((KEYS, HD), jnp.float32), jnp.zeros((KEYS, HD), jnp.float32))
        (dk_sum, dv_sum), dq_all = lax.scan(per_head, start, (q_heads, d_heads))
        return (dq_all, dk_sum, dv_sum)
    dq_g, dk_g, dv_g = lax.map(per_kv, (q_groups, d_groups, k_groups, v_groups))
    dqb = dq_g.transpose(2, 0, 1, 3).reshape(TXT, QH, HD)
    grad_q = dqb * HD ** (-0.5) * q_gain
    dq = rq * grad_q - q * rq ** 3 * lax.optimization_barrier(jnp.mean(q * grad_q, axis=-1, keepdims=True))
    dq_b = dq.reshape(TXT, QH * HD).astype(jnp.bfloat16)
    text_grad = jnp.dot(dq_b, w_query.T, preferred_element_type=jnp.float32)
    grad_k = dk_g.transpose(1, 0, 2) * k_gain
    key_grad = rk * grad_k - k * rk ** 3 * lax.optimization_barrier(jnp.mean(k * grad_k, axis=-1, keepdims=True))
    key_grad = key_grad.reshape(KEYS, KVH * HD)
    value_grad = dv_g.transpose(1, 0, 2).reshape(KEYS, KVH * HD)
    return (text_grad, key_grad, value_grad)
```

```python
import functools

import jax
import jax.numpy as jnp
import numpy as np
from jax import lax
from jax.experimental import pallas as pl
from jax.experimental.pallas import tpu as pltpu
from jax.sharding import PartitionSpec as P

EPS = 1e-05
BLK = 16
MASKED = -1e30
F32 = jnp.float32
BF16 = jnp.bfloat16
NT = (((1,), (1,)), ((), ()))


def dot(a, b, dims=(((1,), (0,)), ((), ()))):
    return lax.dot_general(a, b, dims, preferred_element_type=F32)


def smem():
    return pl.BlockSpec(memory_space=pltpu.SMEM)


def whole(shape):
    return pl.BlockSpec(shape, lambda i: (0,) * len(shape))


def params(**kw):
    return pltpu.CompilerParams(dimension_semantics=("arbitrary",), **kw)


def prep_q(queries, out_grad, q_gain, kv_heads, hd):
    rows, width = queries.shape
    part = width // kv_heads
    scale = hd ** (-0.5)

    def body(q_ref, d_ref, g_ref, *outs):
        gain = g_ref[...]
        for kv in range(kv_heads):
            for j in range(part // hd):
                at = kv * part + j * hd
                q = q_ref[:, at : at + hd].astype(F32)
                r = lax.rsqrt(jnp.mean(q * q, axis=-1, keepdims=True) + EPS)
                outs[kv][:, j * hd : (j + 1) * hd] = (q * r * gain * scale).astype(BF16)
            outs[kv][:, part:] = d_ref[:, kv * part : (kv + 1) * part]

    return pl.pallas_call(
        body,
        grid=(1,),
        in_specs=[whole((rows, width)), whole((rows, width)), whole((1, hd))],
        out_specs=[whole((rows, 2 * part))] * kv_heads,
        out_shape=[jax.ShapeDtypeStruct((rows, 2 * part), BF16)] * kv_heads,
        compiler_params=params(),
        name="prep_q",
    )(queries, out_grad, q_gain)


def prep_k(keys, k_gain, frame_len, kv_heads, hd, kb):
    n = keys.shape[0]
    nb = n // kb

    def body(len_ref, k_ref, g_ref, *outs):
        gain = g_ref[...]
        live = len_ref[0]
        rows = lax.broadcasted_iota(jnp.int32, (n, hd), 0)
        lanes = lax.broadcasted_iota(jnp.int32, (n, hd), 1)
        mask = jnp.where((rows >= live) & (lanes == 0), F32(MASKED), F32(0.0)).astype(BF16)
        for kv in range(kv_heads):
            aug, tr = outs[2 * kv], outs[2 * kv + 1]
            k = k_ref[:, kv * hd : (kv + 1) * hd].astype(F32)
            r = lax.rsqrt(jnp.mean(k * k, axis=-1, keepdims=True) + EPS)
            b = (k * r * gain).astype(BF16)
            aug[:, :hd] = b
            aug[:, hd:] = mask
            for j in range(nb):
                tr[j] = b[j * kb : (j + 1) * kb, :].astype(F32).T.astype(BF16)

    shapes = [(n, 2 * hd), (nb, hd, kb)] * kv_heads
    return pl.pallas_call(
        body,
        grid=(1,),
        in_specs=[smem(), whole(keys.shape), whole((1, hd))],
        out_specs=[whole(s) for s in shapes],
        out_shape=[jax.ShapeDtypeStruct(s, BF16) for s in shapes],
        compiler_params=params(),
        name="prep_k",
    )(frame_len, keys, k_gain)


class Plan:
    def __init__(self, count, rows, group, hd, key_rows):
        self.count, self.rows, self.group, self.hd = count, rows, group, hd
        self.per = rows // BLK
        self.spans = count * self.per
        self.slot = BLK * group
        self.tile = 4
        self.m = self.tile * self.slot
        self.room = -(-self.spans // self.tile) * self.tile * self.slot
        self.key_rows = key_rows
        self.kb = next(key_rows // c for c in (4, 5, 2, 1) if key_rows % (16 * c) == 0)


def stage(plan, me, span_ref, items, qa, ds, lst):
    hd, width = plan.hd, plan.group * plan.hd
    qa[:, hd:] = jnp.ones((qa.shape[0], hd), BF16)
    n = jnp.int32(0)
    for mask in range(plan.count):
        for s in range(plan.per):
            where = (me ^ mask) * plan.per + s
            seen = span_ref[where] > 0

            @pl.when(seen)
            def _(n=n, where=where, mask=mask, s=s):
                lst[n] = where
                for g in range(plan.group):
                    at = pl.ds(pl.multiple_of(n * plan.slot + g * BLK, BLK), BLK)
                    rows = slice(s * BLK, (s + 1) * BLK)
                    qa[at, :hd] = items[mask][rows, g * hd : (g + 1) * hd]
                    ds[at, :] = items[mask][rows, width + g * hd : width + (g + 1) * hd]

            n = n + seen.astype(jnp.int32)
    up = (n + plan.tile - 1) // plan.tile * plan.tile
    for j in range(plan.tile - 1):

        @pl.when(n + j < up)
        def _(j=j):
            lst[n + j] = jnp.int32(plan.spans)
            at = pl.ds(pl.multiple_of((n + j) * plan.slot, BLK), plan.slot)
            qa[at, :hd] = jnp.zeros((plan.slot, hd), BF16)
            ds[at, :] = jnp.zeros((plan.slot, hd), BF16)

    return n, up // plan.tile


def stats_call(plan, meta, span, items, kaug, values, kv):
    hd, kb, m = plan.hd, plan.kb, plan.m
    width = plan.group * hd

    def body(meta_ref, span_ref, *refs):
        its = refs[: plan.count]
        k_ref, v_ref, out, qa, ds, lst = refs[plan.count :]
        n, tiles = stage(plan, meta_ref[0], span_ref, its, qa, ds, lst)
        blocks = (meta_ref[1] + kb - 1) // kb
        out[...] = jnp.zeros(out.shape, F32)

        def tile(t, c):
            at = pl.ds(pl.multiple_of(t * m, m), m)

            def block(b, acc):
                rows = pl.ds(pl.multiple_of(b * kb, 16), kb)
                e = jnp.exp(dot(k_ref[rows, :], qa[at, :], NT))
                dp = dot(v_ref[rows, :], ds[at, :], NT)
                l8 = jnp.sum(e.reshape(kb // 8, 8, m), axis=0)
                u8 = jnp.sum((e * dp).reshape(kb // 8, 8, m), axis=0)
                return acc[0] + l8, acc[1] + u8

            zero = jnp.zeros((8, m), F32)
            l8, u8 = lax.fori_loop(0, blocks, block, (zero, zero))
            tot = jnp.sum(l8, axis=0, keepdims=True)
            wtd = jnp.sum(u8, axis=0, keepdims=True)
            for j in range(plan.tile):

                @pl.when(t * plan.tile + j < n)
                def _(j=j):
                    row = pl.ds(lst[t * plan.tile + j], 1)
                    out[0, row, :] = tot[:, j * plan.slot : (j + 1) * plan.slot]
                    out[1, row, :] = wtd[:, j * plan.slot : (j + 1) * plan.slot]

            return c

        lax.fori_loop(0, tiles, tile, 0)

    flops = 4 * plan.spans * plan.slot * plan.key_rows * hd
    return pl.pallas_call(
        body,
        grid=(1,),
        in_specs=[smem(), smem()]
        + [whole((plan.rows, 2 * width))] * plan.count
        + [whole(kaug.shape), pl.BlockSpec((plan.key_rows, hd), lambda i: (0, kv))],
        out_specs=whole((2, plan.spans, plan.slot)),
        out_shape=jax.ShapeDtypeStruct((2, plan.spans, plan.slot), F32),
        scratch_shapes=[
            pltpu.VMEM((plan.room, 2 * hd), BF16),
            pltpu.VMEM((plan.room, hd), BF16),
            pltpu.SMEM((plan.spans + plan.tile,), jnp.int32),
        ],
        compiler_params=params(vmem_limit_bytes=40 << 20),
        cost_estimate=pl.CostEstimate(flops=flops, transcendentals=0, bytes_accessed=4 << 20),
        name=f"stats{kv}",
    )(meta, span, *items, kaug, values)


def grads_call(plan, meta, span, items, parts, kaug, ktr, keys, values, k_gain, kv, before, order):
    hd, kb, m = plan.hd, plan.kb, plan.m
    width = plan.group * hd
    kv_width = keys.shape[1]
    half = plan.count // 2

    def body(meta_ref, span_ref, *refs):
        its = refs[: plan.count]
        sts = refs[plan.count : plan.count + len(parts)]
        rest = refs[plan.count + len(parts) :]
        k_ref, t_ref, raw_ref, v_ref, g_ref = rest[:5]
        rest = rest[5 + (2 if before else 0) :]
        near, far, kg, vg, qa, ds, dqs, dk, acc, inv, mid, lst = rest
        n, tiles = stage(plan, meta_ref[0], span_ref, its, qa, ds, lst)
        blocks = (meta_ref[1] + kb - 1) // kb
        total = sts[0][0]
        weighted = sts[0][1]
        for st in sts[1:]:
            total = total + st[0]
            weighted = weighted + st[1]
        zero = jnp.zeros((8, plan.slot), F32)
        inv[plan.spans :, :] = zero
        mid[plan.spans :, :] = zero
        inv[: plan.spans, :] = 1.0 / total
        mid[: plan.spans, :] = weighted / total
        dk[...] = jnp.zeros(dk.shape, F32)
        vg[...] = jnp.zeros(vg.shape, F32)

        def tile(t, c):
            at = pl.ds(pl.multiple_of(t * m, m), m)
            rows_of = [pl.ds(lst[t * plan.tile + j], 1) for j in range(plan.tile)]
            r = jnp.concatenate([inv[a, :] for a in rows_of], axis=1)
            x = jnp.concatenate([mid[a, :] for a in rows_of], axis=1)
            acc[...] = jnp.zeros(acc.shape, F32)

            def block(b, c):
                rows = pl.ds(pl.multiple_of(b * kb, 16), kb)
                p = jnp.exp(dot(k_ref[rows, :], qa[at, :], NT)) * r
                dp = dot(v_ref[rows, :], ds[at, :], NT)
                dsb = (p * (dp - x)).astype(BF16)
                pb = p.astype(BF16)
                vg[rows, :] += dot(pb, ds[at, :])
                dk[rows, :] += dot(dsb, qa[at, :hd])
                acc[...] += dot(t_ref[b], dsb)
                return c

            lax.fori_loop(0, blocks, block, 0)
            dqs[at, :] = acc[...].T
            return c

        lax.fori_loop(0, tiles, tile, 0)

        slot = jnp.int32(0)
        for mask in range(plan.count):
            out = far if mask & 1 else near
            base = order.index(mask & ~1) * plan.rows
            for s in range(plan.per):
                seen = span_ref[(meta_ref[0] ^ mask) * plan.per + s] > 0
                rows = slice(base + s * BLK, base + (s + 1) * BLK)

                @pl.when(seen)
                def _(slot=slot, out=out, rows=rows):
                    for g in range(plan.group):
                        at = pl.ds(pl.multiple_of(slot * plan.slot + g * BLK, BLK), BLK)
                        out[rows, g * hd : (g + 1) * hd] = dqs[at, :].astype(out.dtype)

                @pl.when(jnp.logical_not(seen))
                def _(out=out, rows=rows):
                    out[rows, :] = jnp.zeros((BLK, width), out.dtype)

                slot = slot + seen.astype(jnp.int32)

        k = raw_ref[...].astype(F32)
        rk = lax.rsqrt(jnp.mean(k * k, axis=-1, keepdims=True) + EPS)
        g = dk[...] * g_ref[...]
        kg[...] = rk * g - k * rk**3 * jnp.mean(k * g, axis=-1, keepdims=True)

    column = pl.BlockSpec((plan.key_rows, hd), lambda i: (0, kv))
    extra = list(before) if before else []
    n_in = 2 + plan.count + len(parts) + 5
    flops = 10 * plan.spans * plan.slot * plan.key_rows * hd
    return pl.pallas_call(
        body,
        grid=(1,),
        in_specs=[smem(), smem()]
        + [whole((plan.rows, 2 * width))] * plan.count
        + [whole((2, plan.spans, plan.slot))] * len(parts)
        + [whole(kaug.shape), whole(ktr.shape), column, column, whole((1, hd))]
        + [pl.BlockSpec(memory_space=pl.ANY)] * len(extra),
        out_specs=[whole((half * plan.rows, width)), whole((half * plan.rows, width)), column, column],
        out_shape=[
            jax.ShapeDtypeStruct((half * plan.rows, width), F32),
            jax.ShapeDtypeStruct((half * plan.rows, width), BF16),
            jax.ShapeDtypeStruct((plan.key_rows, kv_width), F32),
            jax.ShapeDtypeStruct((plan.key_rows, kv_width), F32),
        ],
        scratch_shapes=[
            pltpu.VMEM((plan.room, 2 * hd), BF16),
            pltpu.VMEM((plan.room, hd), BF16),
            pltpu.VMEM((plan.room, hd), F32),
            pltpu.VMEM((plan.key_rows, hd), F32),
            pltpu.VMEM((hd, m), F32),
            pltpu.VMEM((plan.spans + 8, plan.slot), F32),
            pltpu.VMEM((plan.spans + 8, plan.slot), F32),
            pltpu.SMEM((plan.spans + plan.tile,), jnp.int32),
        ],
        input_output_aliases={n_in: 2, n_in + 1: 3} if before else {},
        compiler_params=params(vmem_limit_bytes=48 << 20),
        cost_estimate=pl.CostEstimate(flops=flops, transcendentals=0, bytes_accessed=8 << 20),
        name=f"grads{kv}",
    )(meta, span, *items, *parts, kaug, ktr, keys, values, k_gain, *extra)


def text_call(tab, keep, recv, queries, q_gain, w_query, prev, prev_at, kv, hd, bn, out_type):
    rows, width = keep.shape
    scale = hd ** (-0.5)
    steps = tab.shape[0]

    def body(tab_ref, keep_ref, recv_ref, q_ref, g_ref, w_ref, *rest):
        out, dq = rest[-2:]

        @pl.when(pl.program_id(0) == 0)
        def _():
            for j in range(width // hd):
                cols = slice(j * hd, (j + 1) * hd)
                g = keep_ref[:, cols] + recv_ref[:, cols].astype(F32)
                g = g * scale * g_ref[...]
                q = q_ref[:, cols].astype(F32)
                r = lax.rsqrt(jnp.mean(q * q, axis=-1, keepdims=True) + EPS)
                x = r * g - q * r**3 * jnp.mean(q * g, axis=-1, keepdims=True)
                dq[:, cols] = x.astype(BF16)

        y = dot(w_ref[...], dq[...], NT).T
        if len(rest) == 3:
            y = y + rest[0][...]
        out[...] = y.astype(out.dtype)

    fixed = lambda shape: pl.BlockSpec(shape, lambda i, t: (0,) * len(shape))
    extra = [] if prev is None else [pl.BlockSpec((rows, bn), lambda i, t: (0, i + prev_at))]
    return pl.pallas_call(
        body,
        grid_spec=pltpu.PrefetchScalarGridSpec(
            num_scalar_prefetch=1,
            grid=(steps,),
            in_specs=[
                fixed((rows, width)),
                fixed((rows, width)),
                pl.BlockSpec((rows, width), lambda i, t: (0, kv)),
                fixed((1, hd)),
                pl.BlockSpec((bn, width), lambda i, t: (t[i], kv)),
            ]
            + extra,
            out_specs=pl.BlockSpec((rows, bn), lambda i, t: (0, i)),
            scratch_shapes=[pltpu.VMEM((rows, width), BF16)],
        ),
        out_shape=jax.ShapeDtypeStruct((rows, steps * bn), out_type),
        compiler_params=params(vmem_limit_bytes=32 << 20),
        cost_estimate=pl.CostEstimate(
            flops=8 * rows * width * steps * bn, transcendentals=0, bytes_accessed=steps * bn * width * 2
        ),
        name=f"text{kv}",
    )(tab, keep, recv, queries, q_gain, w_query, *([] if prev is None else [prev]))


def bits_of(count):
    return [1 << i for i in range(count.bit_length() - 1)]


def split_order(bits):
    if not bits:
        return [0]
    rest = split_order(bits[1:])
    return rest + [bits[0] | r for r in rest]


def swap(x, axis, bit):
    size = lax.axis_size(axis)
    return lax.ppermute(x, axis, [(i, i ^ bit) for i in range(size)])


def local(queries, q_gain, keys, k_gain, values, out_grad, w_query, span_mask, frame_len):
    rows, width = queries.shape
    hd = q_gain.shape[0]
    kv_heads = keys.shape[1] // hd
    part = width // kv_heads
    count = lax.axis_size("frame")
    heads = lax.axis_size("head")
    assert count & (count - 1) == 0 and heads & (heads - 1) == 0 and count > 1
    plan = Plan(count, rows, part // hd, hd, keys.shape[0])
    me = lax.axis_index("frame").astype(jnp.int32)
    meta = jnp.stack([me, frame_len[0]])
    span = span_mask[:, 0]
    q_gain = q_gain.reshape(1, hd)
    k_gain = k_gain.reshape(1, hd)

    own = prep_q(queries, out_grad, q_gain, kv_heads, hd)
    fbits = bits_of(count)
    gathered = []
    for kv in range(kv_heads):
        items = {0: own[kv]}
        for bit in fbits[:0:-1]:
            items.update({m | bit: swap(items[m], "frame", bit) for m in list(items)})
        items.update({m | 1: swap(items[m], "frame", 1) for m in list(items)})
        gathered.append([items[m] for m in range(count)])
    prepared = prep_k(keys, k_gain, frame_len, kv_heads, hd, plan.kb)

    parts = []
    for kv in range(kv_heads):
        st = stats_call(plan, meta, span, gathered[kv], prepared[2 * kv], values, kv)
        st = st + swap(st, "frame", 1)
        parts.append([st] + [swap(st, "frame", m) for m in range(2, count, 2)])

    order = split_order(fbits[1:])
    reduced = []
    before = None
    for kv in range(kv_heads):
        near, far, kg, vg = grads_call(
            plan, meta, span, gathered[kv], parts[kv], prepared[2 * kv], prepared[2 * kv + 1],
            keys, values, k_gain, kv, before, order,
        )
        before = (kg, vg)
        keep, recv = near, swap(far, "frame", 1)
        for bit in fbits[1:]:
            both = keep + recv.astype(F32)
            mid = both.shape[0] // 2
            keep, recv = both[:mid], swap(both[mid:].astype(BF16), "frame", bit)
        reduced.append((keep, recv))

    columns = w_query.shape[0]
    hbits = bits_of(heads)
    flows = min(2, max(1, len(hbits)))
    own_cols = columns // heads
    cw = own_cols // flows
    bn = next(b for b in (512, 256, 128) if cw % b == 0)
    h = lax.axis_index("head").astype(jnp.int32)
    first, second = [], []
    orders = []
    for i in range(flows):
        turn = hbits[i:] + hbits[:i]
        orders.append(turn)
        masks = split_order(turn)
        cut = len(masks) // 2 if turn else 1
        for chosen, into in ((masks[:cut], second), (masks[cut:], first)):
            into += [(m, i * cw // bn + j) for m in chosen for j in range(cw // bn)]
    table = lambda e: (h ^ np.array([m for m, _ in e], np.int32)) * (own_cols // bn) + np.array(
        [o for _, o in e], np.int32
    )
    prev = None
    for kv in range(kv_heads - 1):
        prev = text_call(
            table(first + second), *reduced[kv], queries, q_gain, w_query, prev, 0, kv, hd, bn, F32
        )
    last = functools.partial(
        text_call, keep=reduced[-1][0], recv=reduced[-1][1], queries=queries, q_gain=q_gain,
        w_query=w_query, prev=prev, kv=kv_heads - 1, hd=hd, bn=bn,
    )
    if not hbits:
        text_grad = last(table(second), prev_at=0, out_type=F32)
    else:
        sent = last(table(first), prev_at=0, out_type=BF16)
        per_flow = sent.shape[1] // flows
        moved = [
            swap(sent[:, i * per_flow : (i + 1) * per_flow], "head", orders[i][0])
            for i in range(flows)
        ]
        kept = last(table(second), prev_at=len(first), out_type=F32)
        outs = []
        for i in range(flows):
            both = kept[:, i * per_flow : (i + 1) * per_flow] + moved[i].astype(F32)
            for bit in orders[i][1:]:
                mid = both.shape[1] // 2
                both = both[:, :mid] + swap(both[:, mid:].astype(BF16), "head", bit).astype(F32)
            outs.append(both)
        text_grad = jnp.concatenate(outs, axis=1)
    return (text_grad, kg, vg)


def solution(mesh):
    return jax.shard_map(
        local,
        mesh=mesh,
        in_specs=(
            P("frame", "head"),
            P(),
            P("frame", "head"),
            P(),
            P("frame", "head"),
            P("frame", "head"),
            P(None, "head"),
            P(None, "frame"),
            P("frame"),
        ),
        out_specs=(P("frame", "head"), P("frame", "head"), P("frame", "head")),
        check_vma=False,
    )
```

```python
import functools

import jax
import jax.numpy as jnp
import numpy as np
from jax import lax
from jax.experimental import pallas as pl
from jax.experimental.pallas import tpu as pltpu
from jax.sharding import PartitionSpec as P

EPS = 1e-05
BLK = 16
MASKED = -1e30
TILE = 4
CUTS = (4, 5, 2)
F32 = jnp.float32
BF16 = jnp.bfloat16
NT = (((1,), (1,)), ((), ()))


def dot(a, b, dims=(((1,), (0,)), ((), ()))):
    return lax.dot_general(a, b, dims, preferred_element_type=F32)


def smem():
    return pl.BlockSpec(memory_space=pltpu.SMEM)


def whole(shape):
    return pl.BlockSpec(shape, lambda i: (0,) * len(shape))


def params(**kw):
    return pltpu.CompilerParams(dimension_semantics=("arbitrary",), **kw)


def fixed(shape):
    return pl.BlockSpec(shape, lambda i, s: (0,) * len(shape))


def picked(shape):
    return pl.BlockSpec(shape, lambda i, s: (0, s[0]))


def prep_q(core, queries, out_grad, q_gain, part, hd, own):
    rows = queries.shape[0]
    scale = hd ** (-0.5)

    def body(core_ref, q_ref, d_ref, g_ref, out):
        gain = g_ref[...]
        for j in range(part // hd):
            cols = slice(j * hd, (j + 1) * hd)
            q = q_ref[:, cols].astype(F32)
            r = lax.rsqrt(jnp.mean(q * q, axis=-1, keepdims=True) + EPS)
            out[:, cols] = (q * r * gain * scale).astype(BF16)
        out[:, part:] = d_ref[...]

    left = pl.BlockSpec((rows, part), lambda i, s: (0, 0))
    right = pl.BlockSpec((rows, part), lambda i, s: (0, 1))
    sides = [picked((rows, part)), picked((rows, part))] if own else [left, right]
    return pl.pallas_call(
        body,
        grid_spec=pltpu.PrefetchScalarGridSpec(
            num_scalar_prefetch=1,
            grid=(1,),
            in_specs=[*sides, fixed((1, hd))],
            out_specs=fixed((rows, 2 * part)),
        ),
        out_shape=jax.ShapeDtypeStruct((rows, 2 * part), BF16),
        compiler_params=params(vmem_limit_bytes=8 << 20),
        name="prep_q",
    )(core, queries, out_grad, q_gain)


def prep_k(core, keys, values, got, k_gain, lens, hd, kb):
    n = keys.shape[0]
    nb = n // kb
    pair = 1 if got is None else 2

    def body(core_ref, len_ref, k_ref, v_ref, *refs):
        g_ref, aug, tr, vs, raws = refs[-5:]
        gain = g_ref[...]
        rows = lax.broadcasted_iota(jnp.int32, (n, hd), 0)
        lanes = lax.broadcasted_iota(jnp.int32, (n, hd), 1)
        for fr in range(pair):
            mask = (rows >= len_ref[fr]) & (lanes == 0)
            raw = k_ref[...] if fr == 0 else refs[0][:, :hd]
            k = raw.astype(F32)
            r = lax.rsqrt(jnp.mean(k * k, axis=-1, keepdims=True) + EPS)
            b = (k * r * gain).astype(BF16)
            aug[fr, :, :hd] = b
            aug[fr, :, hd:] = jnp.where(mask, F32(MASKED), F32(0.0)).astype(BF16)
            vs[fr] = v_ref[...] if fr == 0 else refs[0][:, hd:]
            raws[fr] = raw
            for j in range(nb):
                tr[fr, j] = b[j * kb : (j + 1) * kb, :].astype(F32).T.astype(BF16)

    extra = [] if got is None else [got]
    shapes = [(pair, n, 2 * hd), (pair, nb, hd, kb), (pair, n, hd), (pair, n, hd)]
    return pl.pallas_call(
        body,
        grid_spec=pltpu.PrefetchScalarGridSpec(
            num_scalar_prefetch=1,
            grid=(1,),
            in_specs=[smem(), picked((n, hd)), picked((n, hd))]
            + [fixed(x.shape) for x in extra]
            + [fixed((1, hd))],
            out_specs=[fixed(x) for x in shapes],
        ),
        out_shape=[jax.ShapeDtypeStruct(x, BF16) for x in shapes],
        compiler_params=params(vmem_limit_bytes=20 << 20),
        name="prep_k",
    )(core, lens, keys, values, *extra, k_gain)


class Plan:
    def __init__(self, units, rows, group, hd, key_rows, frames):
        self.units, self.rows, self.group, self.hd = units, rows, group, hd
        self.per = rows // BLK
        self.spans = units * self.per
        self.slot = BLK * group
        self.tile = TILE
        self.m = self.tile * self.slot
        self.key_rows, self.frames = key_rows, frames
        self.kb = next(key_rows // c for c in (*CUTS, 1) if key_rows % (16 * c) == 0)

    def staging(self, masks):
        room = (len(masks) * self.per + 1) * self.slot
        spans = len(masks) * self.per + self.tile
        return [
            pltpu.VMEM((room, self.hd), BF16),
            pltpu.VMEM((room, self.hd), BF16),
            pltpu.VMEM((self.m, 2 * self.hd), BF16),
            pltpu.VMEM((self.m, self.hd), BF16),
            pltpu.SMEM((spans,), jnp.int32),
            pltpu.SMEM((spans,), jnp.int32),
        ]


def stage(plan, items, qs, ds, qt):
    hd, width = plan.hd, plan.group * plan.hd
    qt[:, hd:] = jnp.ones((plan.m, hd), BF16)
    for i, item in enumerate(items):
        for s in range(plan.per):
            rows = slice(s * BLK, (s + 1) * BLK)
            for g in range(plan.group):
                at = ((i * plan.per + s) * plan.group + g) * BLK
                qs[at : at + BLK, :] = item[rows, g * hd : (g + 1) * hd]
                ds[at : at + BLK, :] = item[rows, width + g * hd : width + (g + 1) * hd]
    last = len(items) * plan.per * plan.slot
    qs[last:, :] = jnp.zeros((plan.slot, hd), BF16)
    ds[last:, :] = jnp.zeros((plan.slot, hd), BF16)


def visible(plan, masks, fr, me, span_ref, slots, spans):
    n = jnp.int32(0)
    for i, mask in enumerate(masks):
        for s in range(plan.per):
            where = (me ^ mask) * plan.per + s
            slots[n] = jnp.int32(i * plan.per + s)
            spans[n] = where
            n = n + (span_ref[fr * plan.spans + where] > 0).astype(jnp.int32)
    for j in range(plan.tile):
        slots[n + j] = jnp.int32(len(masks) * plan.per)
        spans[n + j] = jnp.int32(plan.spans)
    return n


def fetch(plan, first, size, slots, qs, ds, qt, dt):
    for j in range(size):
        at = pl.ds(pl.multiple_of(slots[first + j] * plan.slot, BLK), plan.slot)
        here = slice(j * plan.slot, (j + 1) * plan.slot)
        qt[here, : plan.hd] = qs[at, :]
        dt[here, :] = ds[at, :]


def over_tiles(plan, n, tile):
    half = plan.tile // 2
    full = (n + half - 1) // plan.tile

    def step(t, c):
        tile(t * plan.tile, plan.tile)
        return c

    lax.fori_loop(0, full, step, 0)

    @pl.when(full * plan.tile < n)
    def _():
        tile(full * plan.tile, half)


def over_blocks(plan, live, block):
    blocks = (live + plan.kb - 1) // plan.kb

    def step(b, c):
        block(2 * b, 2)
        return c

    lax.fori_loop(0, blocks // 2, step, 0)

    @pl.when(blocks % 2 == 1)
    def _():
        block(blocks - 1, 1)


def stats_call(plan, meta, span, masks, items, kaug, vs, prev):
    hd, kb, m = plan.hd, plan.kb, plan.m

    def body(meta_ref, span_ref, *refs):
        its = refs[: len(items)]
        k_ref, v_ref = refs[len(items) : len(items) + 2]
        out, qs, ds, qt, dt, slots, spans, st, acc = refs[-9:]
        stage(plan, its, qs, ds, qt)
        if prev is None:
            st[...] = jnp.zeros(st.shape, F32)
        else:
            st[:, : plan.spans, :] = refs[len(items) + 2][...]

        def frame(fr, c):
            n = visible(plan, masks, fr, meta_ref[0], span_ref, slots, spans)

            def tile(first, size):
                fetch(plan, first, size, slots, qs, ds, qt, dt)
                here = size * plan.slot
                acc[...] = jnp.zeros(acc.shape, F32)

                def block(b, many):
                    rows = pl.ds(pl.multiple_of(b * kb, 16), many * kb)
                    e = jnp.exp(dot(k_ref[fr, rows, :], qt[:here, :], NT))
                    dp = dot(v_ref[fr, rows, :], dt[:here, :], NT)
                    acc[0, :, :here] += jnp.sum(e.reshape(many * kb // 8, 8, here), axis=0)
                    acc[1, :, :here] += jnp.sum((e * dp).reshape(many * kb // 8, 8, here), axis=0)

                over_blocks(plan, meta_ref[1 + fr], block)
                both = jnp.sum(acc[...], axis=1)
                for j in range(size):
                    row = pl.ds(spans[first + j], 1)
                    cols = slice(j * plan.slot, (j + 1) * plan.slot)
                    st[0, row, :] += both[0:1, cols]
                    st[1, row, :] += both[1:2, cols]

            over_tiles(plan, n, tile)
            return c

        lax.fori_loop(0, plan.frames, frame, 0)
        out[...] = st[:, : plan.spans, :]

    flops = 4 * len(masks) * plan.per * plan.slot * plan.key_rows * hd * plan.frames
    shape = (2, plan.spans, plan.slot)
    extra = [] if prev is None else [prev]
    args = [*items, kaug, vs, *extra]
    return pl.pallas_call(
        body,
        grid=(1,),
        in_specs=[smem(), smem()] + [whole(x.shape) for x in args],
        out_specs=whole(shape),
        out_shape=jax.ShapeDtypeStruct(shape, F32),
        scratch_shapes=plan.staging(masks) + [pltpu.VMEM((2, plan.spans + 8, plan.slot), F32), pltpu.VMEM((2, 8, m), F32)],
        compiler_params=params(vmem_limit_bytes=16 << 20),
        cost_estimate=pl.CostEstimate(flops=flops, transcendentals=0, bytes_accessed=4 << 20),
        name="stats",
    )(meta, span, *args)


def grads_call(plan, meta, span, masks, items, parts, kaug, ktr, vs, prev, raw, k_gain, out_type):
    hd, kb, m = plan.hd, plan.kb, plan.m
    width = plan.group * hd
    final = raw is not None

    def body(meta_ref, span_ref, *refs):
        its = refs[: len(items)]
        sts = refs[len(items) : len(items) + len(parts)]
        rest = refs[len(items) + len(parts) :]
        k_ref, t_ref, v_ref = rest[:3]
        dk, dv, qs, ds, qt, dt, slots, spans, dqs, acc, inv, mid = rest[-12:]
        outs = rest[-12 - len(masks) // plan.frames : -12]
        stage(plan, its, qs, ds, qt)
        total = sts[0][0]
        weighted = sts[0][1]
        for st in sts[1:]:
            total = total + st[0]
            weighted = weighted + st[1]
        zero = jnp.zeros((8, plan.slot), F32)
        inv[plan.spans :, :] = zero
        mid[plan.spans :, :] = zero
        inv[: plan.spans, :] = 1.0 / total
        mid[: plan.spans, :] = weighted / total
        dqs[...] = jnp.zeros(dqs.shape, F32)
        if prev is None:
            dk[...] = jnp.zeros(dk.shape, F32)
            dv[...] = jnp.zeros(dv.shape, F32)
        else:
            dk[...] = rest[3][...]
            dv[...] = rest[4][...]

        def frame(fr, c):
            n = visible(plan, masks, fr, meta_ref[0], span_ref, slots, spans)

            def tile(first, size):
                fetch(plan, first, size, slots, qs, ds, qt, dt)
                here = size * plan.slot
                at = [pl.ds(spans[first + j], 1) for j in range(size)]
                r = jnp.concatenate([inv[a, :] for a in at], axis=1)
                x = jnp.concatenate([mid[a, :] for a in at], axis=1)
                acc[...] = jnp.zeros(acc.shape, F32)

                def block(b, many):
                    rows = pl.ds(pl.multiple_of(b * kb, 16), many * kb)
                    p = jnp.exp(dot(k_ref[fr, rows, :], qt[:here, :], NT)) * r
                    dp = dot(v_ref[fr, rows, :], dt[:here, :], NT)
                    dsb = (p * (dp - x)).astype(BF16)
                    pb = p.astype(BF16)
                    dv[fr, rows, :] += dot(pb, dt[:here, :])
                    dk[fr, rows, :] += dot(dsb, qt[:here, :hd])
                    y = dot(t_ref[fr, b], dsb[:kb])
                    for i in range(1, many):
                        y = y + dot(t_ref[fr, b + i], dsb[i * kb : (i + 1) * kb])
                    acc[:, :here] += y

                over_blocks(plan, meta_ref[1 + fr], block)
                y = acc[...].T
                for j in range(size):
                    s = pl.ds(pl.multiple_of(slots[first + j] * plan.slot, BLK), plan.slot)
                    dqs[s, :] += y[j * plan.slot : (j + 1) * plan.slot, :]

            over_tiles(plan, n, tile)
            return c

        lax.fori_loop(0, plan.frames, frame, 0)
        share = plan.per * plan.frames
        for i, out in enumerate(outs):
            for s in range(share):
                for g in range(plan.group):
                    at = ((i * share + s) * plan.group + g) * BLK
                    rows = slice(s * BLK, (s + 1) * BLK)
                    out[rows, g * hd : (g + 1) * hd] = dqs[at : at + BLK, :].astype(out_type)
        if final:
            raw_ref, g_ref = rest[5:7]
            for fr in range(plan.frames):
                k = raw_ref[fr].astype(F32)
                rk = lax.rsqrt(jnp.mean(k * k, axis=-1, keepdims=True) + EPS)
                g = dk[fr] * g_ref[...]
                dk[fr] = rk * g - k * rk**3 * jnp.mean(k * g, axis=-1, keepdims=True)

    args = [*items, *parts, kaug, ktr, vs] + (list(prev) if prev else []) + ([raw, k_gain] if final else [])
    flops = 10 * len(masks) * plan.per * plan.slot * plan.key_rows * hd * plan.frames
    out = jax.ShapeDtypeStruct((plan.frames * plan.rows, width), out_type)
    shapes = [out] * (len(masks) // plan.frames) + [
        jax.ShapeDtypeStruct((plan.frames, plan.key_rows, hd), F32),
        jax.ShapeDtypeStruct((plan.frames, plan.key_rows, hd), F32),
    ]
    return pl.pallas_call(
        body,
        grid=(1,),
        in_specs=[smem(), smem()] + [whole(x.shape) for x in args],
        out_specs=[whole(x.shape) for x in shapes],
        out_shape=shapes,
        scratch_shapes=plan.staging(masks)
        + [
            pltpu.VMEM(((len(masks) * plan.per + 1) * plan.slot, hd), F32),
            pltpu.VMEM((hd, m), F32),
            pltpu.VMEM((plan.spans + 8, plan.slot), F32),
            pltpu.VMEM((plan.spans + 8, plan.slot), F32),
        ],
        compiler_params=params(vmem_limit_bytes=28 << 20),
        cost_estimate=pl.CostEstimate(flops=flops, transcendentals=0, bytes_accessed=8 << 20),
        name="grads_last" if final else "grads",
    )(meta, span, *args)


def text_call(tab, keep, recvs, queries, got, q_gain, w_query, pair, bn, types, hd):
    rows, width = keep.shape
    scale = hd ** (-0.5)
    steps = tab.shape[0] - 1
    mine = rows // pair
    ways = 4
    bw = bn // ways

    def body(tab_ref, keep_ref, *rest):
        recv_refs = rest[: len(recvs)]
        q_refs = rest[len(recvs) : len(recvs) + pair]
        rest = rest[len(recvs) + pair :]
        g_ref, w_refs, outs, dq = rest[0], rest[1 : 1 + ways], rest[1 + ways : -1], rest[-1]

        @pl.when(pl.program_id(0) == 0)
        def _():
            for i, q_ref in enumerate(q_refs):
                at = slice(i * mine, (i + 1) * mine)
                for j in range(width // hd):
                    cols = slice(j * hd, (j + 1) * hd)
                    g = keep_ref[at, cols]
                    for recv_ref in recv_refs:
                        g = g + recv_ref[at, cols].astype(F32)
                    g = g * scale * g_ref[...]
                    q = q_ref[:, cols].astype(F32)
                    r = lax.rsqrt(jnp.mean(q * q, axis=-1, keepdims=True) + EPS)
                    x = r * g - q * r**3 * jnp.mean(q * g, axis=-1, keepdims=True)
                    dq[at, cols] = x.astype(BF16)

        for j, w_ref in enumerate(w_refs):
            y = dot(w_ref[...], dq[...], NT).T
            for i, out in enumerate(outs):
                out[:, j * bw : (j + 1) * bw] = y[i * mine : (i + 1) * mine, :].astype(types[i])

    extra = [] if pair == 1 else [got]
    return pl.pallas_call(
        body,
        grid_spec=pltpu.PrefetchScalarGridSpec(
            num_scalar_prefetch=1,
            grid=(steps,),
            in_specs=[
                *[fixed((rows, width))] * (len(recvs) + 1),
                picked((mine, width)),
                *[fixed((mine, width)) for _ in extra],
                fixed((1, hd)),
                *[
                    pl.BlockSpec((bw, width), lambda i, t, j=j: (t[i + 1] * ways + j, t[0]))
                    for j in range(ways)
                ],
            ],
            out_specs=[pl.BlockSpec((mine, bn), lambda i, t: (0, i))] * pair,
            scratch_shapes=[pltpu.VMEM((rows, width), BF16)],
        ),
        out_shape=[jax.ShapeDtypeStruct((mine, steps * bn), types[i]) for i in range(pair)],
        compiler_params=params(vmem_limit_bytes=24 << 20),
        cost_estimate=pl.CostEstimate(
            flops=8 * rows * width * steps * bn, transcendentals=0, bytes_accessed=steps * bn * width * 2
        ),
        name="text",
    )(tab, keep, *recvs, queries, *extra, q_gain, *[w_query] * ways)


def bits_of(count):
    return [1 << i for i in range(count.bit_length() - 1)]


def split_order(bits):
    if not bits:
        return [0]
    rest = split_order(bits[1:])
    return rest + [bits[0] | r for r in rest]


def swap(x, axis, bit):
    size = lax.axis_size(axis)
    return lax.ppermute(x, axis, [(i, i ^ bit) for i in range(size)])


def local(queries, q_gain, keys, k_gain, values, out_grad, w_query, span_mask, frame_len):
    rows, width = queries.shape
    hd = q_gain.shape[0]
    kv_heads = keys.shape[1] // hd
    part = width // kv_heads
    count = lax.axis_size("frame")
    heads = lax.axis_size("head")
    assert count & (count - 1) == 0 and heads & (heads - 1) == 0 and count > 2 * (keys.shape[1] // q_gain.shape[0])
    assert kv_heads in (1, 2)
    pair = kv_heads
    units = count // pair
    me = lax.axis_index("frame").astype(jnp.int32)
    core = (me % pair).reshape(1)
    plan = Plan(count, rows, part // hd, hd, keys.shape[0], pair)
    span = span_mask[:, 0]
    q_gain = q_gain.reshape(1, hd)
    k_gain = k_gain.reshape(1, hd)

    items = {0: prep_q(core, queries, out_grad, q_gain, part, hd, True)}
    got_q = got_k = None
    if pair == 2:
        other = lambda x, w: lax.dynamic_slice_in_dim(x, (1 - core[0]) * w, w, axis=1)
        got_q = swap(jnp.concatenate([other(queries, part), other(out_grad, part)], axis=1), "frame", 1)
        ints = swap(jnp.concatenate([span, frame_len]), "frame", 1)
        got_k = swap(jnp.concatenate([other(keys, hd), other(values, hd)], axis=1), "frame", 1)
        span = jnp.concatenate([span, ints[:-1]])
        frame_len = jnp.concatenate([frame_len, ints[-1:]])
        items[1] = prep_q(core, got_q, got_q, q_gain, part, hd, False)
    meta = jnp.concatenate([me.reshape(1), frame_len])

    kaug, ktr, vs, raw_k = prep_k(core, keys, values, got_k, k_gain, frame_len, hd, plan.kb)
    ours = lambda masks: [m * pair + i for m in masks for i in range(pair)]
    stats = lambda masks, prev: stats_call(
        plan, meta, span, ours(masks), [items[m] for m in ours(masks)], kaug, vs, prev
    )
    for bit in bits_of(units)[:0:-1]:
        step = bit * pair
        items.update({m | step: swap(items[m], "frame", step) for m in sorted(items)})
    items.update({m | pair: swap(items[m], "frame", pair) for m in ours([0])})
    st = stats([0], None)
    far = list(range(2, units, 2))
    held = lax.optimization_barrier((st, *[items[m] for m in ours(far)]))
    st = held[0]
    items.update(zip(ours(far), held[1:]))
    items.update({m | pair: swap(items[m], "frame", pair) for m in ours(far)})
    st = stats(far + [1], st)
    st = stats([m | 1 for m in far], st)
    parts = [st] + [swap(st, "frame", m * pair) for m in range(1, units)]

    recvs = []
    prev = None
    for masks in (list(range(2, units)), [1], [0]):
        final = masks == [0]
        *dqs, dk, dv = grads_call(
            plan, meta, span, ours(masks), [items[m] for m in ours(masks)], parts, kaug, ktr, vs, prev,
            *((raw_k, k_gain, F32) if final else (None, None, BF16)),
        )
        prev = (dk, dv)
        if not final:
            recvs += [swap(x, "frame", m * pair) for x, m in zip(dqs, masks)]
    keep, kg, vg = dqs[0], dk, dv
    if pair == 2:
        join = lambda a, b: jnp.where(
            core[0] == 0, jnp.concatenate([a, b], axis=1), jnp.concatenate([b, a], axis=1)
        )
        kg = join(kg[0], swap(kg[1], "frame", 1))
        vg = join(vg[0], swap(vg[1], "frame", 1))
    else:
        kg, vg = kg[0], vg[0]
    columns = w_query.shape[0]
    hbits = bits_of(heads)
    flows = min(2, max(1, len(hbits)))
    own_cols = columns // heads
    cw = own_cols // flows
    bn = next(b for b in (1024, 512, 256, 128) if cw % b == 0)
    h = lax.axis_index("head").astype(jnp.int32)
    first, second = [], []
    turns = []
    for i in range(flows):
        turn = hbits[i:] + hbits[:i]
        turns.append(turn)
        masks = split_order(turn)
        cut = len(masks) // 2 if turn else 1
        for chosen, into in ((masks[:cut], second), (masks[cut:], first)):
            into += [(m, i * cw // bn + j) for m in chosen for j in range(cw // bn)]

    def text(entries, kind):
        where = (h ^ np.array([m for m, _ in entries], np.int32)) * (own_cols // bn)
        tab = jnp.concatenate([core, where + np.array([o for _, o in entries], np.int32)])
        return text_call(tab, keep, recvs, queries, got_q, q_gain, w_query, pair, bn, (kind, BF16), hd)

    whole_of = lambda y: y[0] if pair == 1 else y[0] + swap(y[1], "frame", 1).astype(F32)
    pieces = lambda y: [y[:, i * y.shape[1] // flows : (i + 1) * y.shape[1] // flows] for i in range(flows)]
    moved = []
    if hbits:
        sums = pieces(whole_of(text(first, F32)))
        moved = [swap(s.astype(BF16), "head", t[0]) for s, t in zip(sums, turns)]
    outs = []
    for i, both in enumerate(pieces(whole_of(text(second, F32)))):
        if hbits:
            both = both + moved[i].astype(F32)
        for bit in turns[i][1:]:
            mid = both.shape[1] // 2
            both = both[:, :mid] + swap(both[:, mid:].astype(BF16), "head", bit).astype(F32)
        outs.append(both)
    return (jnp.concatenate(outs, axis=1), kg, vg)


def solution(mesh):
    return jax.shard_map(
        local,
        mesh=mesh,
        in_specs=(
            P("frame", "head"),
            P(),
            P("frame", "head"),
            P(),
            P("frame", "head"),
            P("frame", "head"),
            P(None, "head"),
            P(None, "frame"),
            P("frame"),
        ),
        out_specs=(P("frame", "head"), P("frame", "head"), P("frame", "head")),
        check_vma=False,
    )
```

```python
import functools

import jax
import jax.numpy as jnp
import numpy as np
from jax import lax
from jax.experimental import pallas as pl
from jax.experimental.pallas import tpu as pltpu
from jax.sharding import PartitionSpec as P

EPS = 1e-05
BLK = 16
MASKED = -1e30
TILE = 4
CUTS = (4, 5, 2)
F32 = jnp.float32
BF16 = jnp.bfloat16
NT = (((1,), (1,)), ((), ()))


def dot(a, b, dims=(((1,), (0,)), ((), ()))):
    return lax.dot_general(a, b, dims, preferred_element_type=F32)


def smem():
    return pl.BlockSpec(memory_space=pltpu.SMEM)


def whole(shape):
    return pl.BlockSpec(shape, lambda i: (0,) * len(shape))


def params(**kw):
    return pltpu.CompilerParams(dimension_semantics=("arbitrary",), **kw)


def fixed(shape):
    return pl.BlockSpec(shape, lambda i, s: (0,) * len(shape))


def picked(shape):
    return pl.BlockSpec(shape, lambda i, s: (0, s[0]))


def prep_q(core, queries, out_grad, q_gain, part, hd, own):
    rows = queries.shape[0]
    scale = hd ** (-0.5)

    def body(core_ref, q_ref, d_ref, g_ref, out):
        gain = g_ref[...]
        for j in range(part // hd):
            cols = slice(j * hd, (j + 1) * hd)
            q = q_ref[:, cols].astype(F32)
            r = lax.rsqrt(jnp.mean(q * q, axis=-1, keepdims=True) + EPS)
            out[:, cols] = (q * r * gain * scale).astype(BF16)
        out[:, part:] = d_ref[...]

    left = pl.BlockSpec((rows, part), lambda i, s: (0, 0))
    right = pl.BlockSpec((rows, part), lambda i, s: (0, 1))
    sides = [picked((rows, part)), picked((rows, part))] if own else [left, right]
    return pl.pallas_call(
        body,
        grid_spec=pltpu.PrefetchScalarGridSpec(
            num_scalar_prefetch=1,
            grid=(1,),
            in_specs=[*sides, fixed((1, hd))],
            out_specs=fixed((rows, 2 * part)),
        ),
        out_shape=jax.ShapeDtypeStruct((rows, 2 * part), BF16),
        compiler_params=params(vmem_limit_bytes=8 << 20),
        name="prep_q",
    )(core, queries, out_grad, q_gain)


def prep_k(core, keys, values, got, k_gain, lens, hd, kb):
    n = keys.shape[0]
    nb = n // kb
    pair = 1 if got is None else 2

    def body(core_ref, len_ref, k_ref, v_ref, *refs):
        g_ref, aug, tr, vs, raws = refs[-5:]
        gain = g_ref[...]
        rows = lax.broadcasted_iota(jnp.int32, (n, hd), 0)
        lanes = lax.broadcasted_iota(jnp.int32, (n, hd), 1)
        for fr in range(pair):
            mask = (rows >= len_ref[fr]) & (lanes == 0)
            raw = k_ref[...] if fr == 0 else refs[0][:, :hd]
            k = raw.astype(F32)
            r = lax.rsqrt(jnp.mean(k * k, axis=-1, keepdims=True) + EPS)
            b = (k * r * gain).astype(BF16)
            aug[fr, :, :hd] = b
            aug[fr, :, hd:] = jnp.where(mask, F32(MASKED), F32(0.0)).astype(BF16)
            vs[fr] = v_ref[...] if fr == 0 else refs[0][:, hd:]
            raws[fr] = raw
            for j in range(nb):
                tr[fr, j] = b[j * kb : (j + 1) * kb, :].astype(F32).T.astype(BF16)

    extra = [] if got is None else [got]
    shapes = [(pair, n, 2 * hd), (pair, nb, hd, kb), (pair, n, hd), (pair, n, hd)]
    return pl.pallas_call(
        body,
        grid_spec=pltpu.PrefetchScalarGridSpec(
            num_scalar_prefetch=1,
            grid=(1,),
            in_specs=[smem(), picked((n, hd)), picked((n, hd))]
            + [fixed(x.shape) for x in extra]
            + [fixed((1, hd))],
            out_specs=[fixed(x) for x in shapes],
        ),
        out_shape=[jax.ShapeDtypeStruct(x, BF16) for x in shapes],
        compiler_params=params(vmem_limit_bytes=20 << 20),
        name="prep_k",
    )(core, lens, keys, values, *extra, k_gain)


class Plan:
    def __init__(self, units, rows, group, hd, key_rows, frames):
        self.units, self.rows, self.group, self.hd = units, rows, group, hd
        self.per = rows // BLK
        self.spans = units * self.per
        self.slot = BLK * group
        self.tile = TILE
        self.m = self.tile * self.slot
        self.key_rows, self.frames = key_rows, frames
        self.kb = next(key_rows // c for c in (*CUTS, 1) if key_rows % (16 * c) == 0)

    def staging(self, masks):
        room = (len(masks) * self.per + 1) * self.slot
        spans = len(masks) * self.per + self.tile
        return [
            pltpu.VMEM((room, self.hd), BF16),
            pltpu.VMEM((room, self.hd), BF16),
            pltpu.VMEM((self.m, 2 * self.hd), BF16),
            pltpu.VMEM((self.m, self.hd), BF16),
            pltpu.SMEM((spans,), jnp.int32),
            pltpu.SMEM((spans,), jnp.int32),
        ]


def stage(plan, items, qs, ds, qt):
    hd, width = plan.hd, plan.group * plan.hd
    qt[:, hd:] = jnp.ones((plan.m, hd), BF16)
    for i, item in enumerate(items):
        for s in range(plan.per):
            rows = slice(s * BLK, (s + 1) * BLK)
            for g in range(plan.group):
                at = ((i * plan.per + s) * plan.group + g) * BLK
                qs[at : at + BLK, :] = item[rows, g * hd : (g + 1) * hd]
                ds[at : at + BLK, :] = item[rows, width + g * hd : width + (g + 1) * hd]
    last = len(items) * plan.per * plan.slot
    qs[last:, :] = jnp.zeros((plan.slot, hd), BF16)
    ds[last:, :] = jnp.zeros((plan.slot, hd), BF16)


def visible(plan, masks, fr, me, span_ref, slots, spans):
    n = jnp.int32(0)
    for i, mask in enumerate(masks):
        for s in range(plan.per):
            where = (me ^ mask) * plan.per + s
            slots[n] = jnp.int32(i * plan.per + s)
            spans[n] = where
            n = n + (span_ref[fr * plan.spans + where] > 0).astype(jnp.int32)
    for j in range(plan.tile):
        slots[n + j] = jnp.int32(len(masks) * plan.per)
        spans[n + j] = jnp.int32(plan.spans)
    return n


def fetch(plan, first, size, slots, qs, ds, qt, dt):
    for j in range(size):
        at = pl.ds(pl.multiple_of(slots[first + j] * plan.slot, BLK), plan.slot)
        here = slice(j * plan.slot, (j + 1) * plan.slot)
        qt[here, : plan.hd] = qs[at, :]
        dt[here, :] = ds[at, :]


def over_tiles(plan, n, tile):
    half = plan.tile // 2
    full = (n + half - 1) // plan.tile

    def step(t, c):
        tile(t * plan.tile, plan.tile)
        return c

    lax.fori_loop(0, full, step, 0)

    @pl.when(full * plan.tile < n)
    def _():
        tile(full * plan.tile, half)


def over_blocks(plan, live, block):
    blocks = (live + plan.kb - 1) // plan.kb

    def step(b, c):
        block(2 * b, 2)
        return c

    lax.fori_loop(0, blocks // 2, step, 0)

    @pl.when(blocks % 2 == 1)
    def _():
        block(blocks - 1, 1)


def stats_call(plan, meta, span, masks, items, kaug, vs, prev):
    hd, kb, m = plan.hd, plan.kb, plan.m

    def body(meta_ref, span_ref, *refs):
        its = refs[: len(items)]
        k_ref, v_ref = refs[len(items) : len(items) + 2]
        out, qs, ds, qt, dt, slots, spans, st, acc = refs[-9:]
        stage(plan, its, qs, ds, qt)
        if prev is None:
            st[...] = jnp.zeros(st.shape, F32)
        else:
            st[:, : plan.spans, :] = refs[len(items) + 2][...]

        def frame(fr, c):
            n = visible(plan, masks, fr, meta_ref[0], span_ref, slots, spans)

            def tile(first, size):
                fetch(plan, first, size, slots, qs, ds, qt, dt)
                here = size * plan.slot
                acc[...] = jnp.zeros(acc.shape, F32)

                def block(b, many):
                    rows = pl.ds(pl.multiple_of(b * kb, 16), many * kb)
                    e = jnp.exp(dot(k_ref[fr, rows, :], qt[:here, :], NT))
                    dp = dot(v_ref[fr, rows, :], dt[:here, :], NT)
                    acc[0, :, :here] += jnp.sum(e.reshape(many * kb // 8, 8, here), axis=0)
                    acc[1, :, :here] += jnp.sum((e * dp).reshape(many * kb // 8, 8, here), axis=0)

                over_blocks(plan, meta_ref[1 + fr], block)
                both = jnp.sum(acc[...], axis=1)
                for j in range(size):
                    row = pl.ds(spans[first + j], 1)
                    cols = slice(j * plan.slot, (j + 1) * plan.slot)
                    st[0, row, :] += both[0:1, cols]
                    st[1, row, :] += both[1:2, cols]

            over_tiles(plan, n, tile)
            return c

        lax.fori_loop(0, plan.frames, frame, 0)
        out[...] = st[:, : plan.spans, :]

    flops = 4 * len(masks) * plan.per * plan.slot * plan.key_rows * hd * plan.frames
    shape = (2, plan.spans, plan.slot)
    extra = [] if prev is None else [prev]
    args = [*items, kaug, vs, *extra]
    return pl.pallas_call(
        body,
        grid=(1,),
        in_specs=[smem(), smem()] + [whole(x.shape) for x in args],
        out_specs=whole(shape),
        out_shape=jax.ShapeDtypeStruct(shape, F32),
        scratch_shapes=plan.staging(masks) + [pltpu.VMEM((2, plan.spans + 8, plan.slot), F32), pltpu.VMEM((2, 8, m), F32)],
        compiler_params=params(vmem_limit_bytes=16 << 20),
        cost_estimate=pl.CostEstimate(flops=flops, transcendentals=0, bytes_accessed=4 << 20),
        name="stats",
    )(meta, span, *args)


def grads_call(plan, meta, span, masks, items, parts, kaug, ktr, vs, prev, raw, k_gain, out_type):
    hd, kb, m = plan.hd, plan.kb, plan.m
    width = plan.group * hd
    final = raw is not None

    def body(meta_ref, span_ref, *refs):
        its = refs[: len(items)]
        sts = refs[len(items) : len(items) + len(parts)]
        rest = refs[len(items) + len(parts) :]
        k_ref, t_ref, v_ref = rest[:3]
        dk, dv, qs, ds, qt, dt, slots, spans, dqs, acc, inv, mid = rest[-12:]
        outs = rest[-12 - len(masks) // plan.frames : -12]
        stage(plan, its, qs, ds, qt)
        total = sts[0][0]
        weighted = sts[0][1]
        for st in sts[1:]:
            total = total + st[0]
            weighted = weighted + st[1]
        zero = jnp.zeros((8, plan.slot), F32)
        inv[plan.spans :, :] = zero
        mid[plan.spans :, :] = zero
        inv[: plan.spans, :] = 1.0 / total
        mid[: plan.spans, :] = weighted / total
        dqs[...] = jnp.zeros(dqs.shape, F32)
        if prev is None:
            dk[...] = jnp.zeros(dk.shape, F32)
            dv[...] = jnp.zeros(dv.shape, F32)
        else:
            dk[...] = rest[3][...]
            dv[...] = rest[4][...]

        def frame(fr, c):
            n = visible(plan, masks, fr, meta_ref[0], span_ref, slots, spans)

            def tile(first, size):
                fetch(plan, first, size, slots, qs, ds, qt, dt)
                here = size * plan.slot
                at = [pl.ds(spans[first + j], 1) for j in range(size)]
                r = jnp.concatenate([inv[a, :] for a in at], axis=1)
                x = jnp.concatenate([mid[a, :] for a in at], axis=1)
                acc[...] = jnp.zeros(acc.shape, F32)

                def block(b, many):
                    rows = pl.ds(pl.multiple_of(b * kb, 16), many * kb)
                    p = jnp.exp(dot(k_ref[fr, rows, :], qt[:here, :], NT)) * r
                    dp = dot(v_ref[fr, rows, :], dt[:here, :], NT)
                    dsb = (p * (dp - x)).astype(BF16)
                    pb = p.astype(BF16)
                    dv[fr, rows, :] += dot(pb, dt[:here, :])
                    dk[fr, rows, :] += dot(dsb, qt[:here, :hd])
                    y = dot(t_ref[fr, b], dsb[:kb])
                    for i in range(1, many):
                        y = y + dot(t_ref[fr, b + i], dsb[i * kb : (i + 1) * kb])
                    acc[:, :here] += y

                over_blocks(plan, meta_ref[1 + fr], block)
                y = acc[...].T
                for j in range(size):
                    s = pl.ds(pl.multiple_of(slots[first + j] * plan.slot, BLK), plan.slot)
                    dqs[s, :] += y[j * plan.slot : (j + 1) * plan.slot, :]

            over_tiles(plan, n, tile)
            return c

        lax.fori_loop(0, plan.frames, frame, 0)
        share = plan.per * plan.frames
        for i, out in enumerate(outs):
            for s in range(share):
                for g in range(plan.group):
                    at = ((i * share + s) * plan.group + g) * BLK
                    rows = slice(s * BLK, (s + 1) * BLK)
                    out[rows, g * hd : (g + 1) * hd] = dqs[at : at + BLK, :].astype(out_type)
        if final:
            raw_ref, g_ref = rest[5:7]
            for fr in range(plan.frames):
                k = raw_ref[fr].astype(F32)
                rk = lax.rsqrt(jnp.mean(k * k, axis=-1, keepdims=True) + EPS)
                g = dk[fr] * g_ref[...]
                dk[fr] = rk * g - k * rk**3 * jnp.mean(k * g, axis=-1, keepdims=True)

    args = [*items, *parts, kaug, ktr, vs] + (list(prev) if prev else []) + ([raw, k_gain] if final else [])
    flops = 10 * len(masks) * plan.per * plan.slot * plan.key_rows * hd * plan.frames
    out = jax.ShapeDtypeStruct((plan.frames * plan.rows, width), out_type)
    shapes = [out] * (len(masks) // plan.frames) + [
        jax.ShapeDtypeStruct((plan.frames, plan.key_rows, hd), F32),
        jax.ShapeDtypeStruct((plan.frames, plan.key_rows, hd), F32),
    ]
    return pl.pallas_call(
        body,
        grid=(1,),
        in_specs=[smem(), smem()] + [whole(x.shape) for x in args],
        out_specs=[whole(x.shape) for x in shapes],
        out_shape=shapes,
        scratch_shapes=plan.staging(masks)
        + [
            pltpu.VMEM(((len(masks) * plan.per + 1) * plan.slot, hd), F32),
            pltpu.VMEM((hd, m), F32),
            pltpu.VMEM((plan.spans + 8, plan.slot), F32),
            pltpu.VMEM((plan.spans + 8, plan.slot), F32),
        ],
        compiler_params=params(vmem_limit_bytes=20 << 20),
        cost_estimate=pl.CostEstimate(flops=flops, transcendentals=0, bytes_accessed=8 << 20),
        name="grads_last" if final else "grads",
    )(meta, span, *args)


def text_call(tab, keep, recvs, queries, got, q_gain, w_query, pair, bn, types, hd, after):
    rows, width = keep.shape
    scale = hd ** (-0.5)
    steps = tab.shape[0] - 1
    mine = rows // pair
    ways = 4
    bw = bn // ways

    def body(tab_ref, keep_ref, *rest):
        recv_refs = rest[: len(recvs)]
        q_refs = rest[len(recvs) : len(recvs) + pair]
        rest = rest[len(recvs) + pair :]
        g_ref, w_refs, outs, dq = rest[0], rest[1 : 1 + ways], rest[1 + ways + len(after) : -1], rest[-1]

        @pl.when(pl.program_id(0) == 0)
        def _():
            for i, q_ref in enumerate(q_refs):
                at = slice(i * mine, (i + 1) * mine)
                for j in range(width // hd):
                    cols = slice(j * hd, (j + 1) * hd)
                    g = keep_ref[at, cols]
                    for recv_ref in recv_refs:
                        g = g + recv_ref[at, cols].astype(F32)
                    g = g * scale * g_ref[...]
                    q = q_ref[:, cols].astype(F32)
                    r = lax.rsqrt(jnp.mean(q * q, axis=-1, keepdims=True) + EPS)
                    x = r * g - q * r**3 * jnp.mean(q * g, axis=-1, keepdims=True)
                    dq[at, cols] = x.astype(BF16)

        for j, w_ref in enumerate(w_refs):
            y = dot(w_ref[...], dq[...], NT).T
            for i, out in enumerate(outs):
                out[:, j * bw : (j + 1) * bw] = y[i * mine : (i + 1) * mine, :].astype(types[i])

    extra = [] if pair == 1 else [got]
    return pl.pallas_call(
        body,
        grid_spec=pltpu.PrefetchScalarGridSpec(
            num_scalar_prefetch=1,
            grid=(steps,),
            in_specs=[
                *[fixed((rows, width))] * (len(recvs) + 1),
                picked((mine, width)),
                *[fixed((mine, width)) for _ in extra],
                fixed((1, hd)),
                *[
                    pl.BlockSpec((bw, width), lambda i, t, j=j: (t[i + 1] * ways + j, t[0]))
                    for j in range(ways)
                ],
                *[pl.BlockSpec(memory_space=pl.ANY) for _ in after],
            ],
            out_specs=[pl.BlockSpec((mine, bn), lambda i, t: (0, i))] * pair,
            scratch_shapes=[pltpu.VMEM((rows, width), BF16)],
        ),
        out_shape=[jax.ShapeDtypeStruct((mine, steps * bn), types[i]) for i in range(pair)],
        compiler_params=params(vmem_limit_bytes=24 << 20),
        cost_estimate=pl.CostEstimate(
            flops=8 * rows * width * steps * bn, transcendentals=0, bytes_accessed=steps * bn * width * 2
        ),
        name="text",
    )(tab, keep, *recvs, queries, *extra, q_gain, *[w_query] * ways, *after)


def bits_of(count):
    return [1 << i for i in range(count.bit_length() - 1)]


def split_order(bits):
    if not bits:
        return [0]
    rest = split_order(bits[1:])
    return rest + [bits[0] | r for r in rest]


def swap(x, axis, bit):
    size = lax.axis_size(axis)
    return lax.ppermute(x, axis, [(i, i ^ bit) for i in range(size)])


def local(queries, q_gain, keys, k_gain, values, out_grad, w_query, span_mask, frame_len):
    rows, width = queries.shape
    hd = q_gain.shape[0]
    kv_heads = keys.shape[1] // hd
    part = width // kv_heads
    count = lax.axis_size("frame")
    heads = lax.axis_size("head")
    assert count & (count - 1) == 0 and heads & (heads - 1) == 0 and count > 2 * (keys.shape[1] // q_gain.shape[0])
    assert kv_heads in (1, 2)
    pair = kv_heads
    units = count // pair
    me = lax.axis_index("frame").astype(jnp.int32)
    core = (me % pair).reshape(1)
    plan = Plan(count, rows, part // hd, hd, keys.shape[0], pair)
    span = span_mask[:, 0]
    q_gain = q_gain.reshape(1, hd)
    k_gain = k_gain.reshape(1, hd)

    items = {0: prep_q(core, queries, out_grad, q_gain, part, hd, True)}
    got_q = got_k = None
    if pair == 2:
        other = lambda x, w: lax.dynamic_slice_in_dim(x, (1 - core[0]) * w, w, axis=1)
        got_q = swap(jnp.concatenate([other(queries, part), other(out_grad, part)], axis=1), "frame", 1)
        ints = swap(jnp.concatenate([span, frame_len]), "frame", 1)
        got_k = swap(jnp.concatenate([other(keys, hd), other(values, hd)], axis=1), "frame", 1)
        span = jnp.concatenate([span, ints[:-1]])
        frame_len = jnp.concatenate([frame_len, ints[-1:]])
        items[1] = prep_q(core, got_q, got_q, q_gain, part, hd, False)
    meta = jnp.concatenate([me.reshape(1), frame_len])

    kaug, ktr, vs, raw_k = prep_k(core, keys, values, got_k, k_gain, frame_len, hd, plan.kb)
    ours = lambda masks: [m * pair + i for m in masks for i in range(pair)]
    stats = lambda masks, prev: stats_call(
        plan, meta, span, ours(masks), [items[m] for m in ours(masks)], kaug, vs, prev
    )
    for bit in bits_of(units)[:0:-1]:
        step = bit * pair
        items.update({m | step: swap(items[m], "frame", step) for m in sorted(items)})
    items.update({m | pair: swap(items[m], "frame", pair) for m in ours([0])})
    st = stats([0], None)
    far = list(range(2, units, 2))
    held = lax.optimization_barrier((st, *[items[m] for m in ours(far)]))
    st = held[0]
    items.update(zip(ours(far), held[1:]))
    items.update({m | pair: swap(items[m], "frame", pair) for m in ours(far)})
    st = stats(far + [1], st)
    st = stats([m | 1 for m in far], st)
    parts = [st] + [swap(st, "frame", m * pair) for m in range(1, units)]

    recvs, prev, met = [], None, {}
    for masks in (list(range(1, units, 2)), far, [0]):
        final = masks == [0]
        *dqs, dk, dv = grads_call(
            plan, meta, span, ours(masks), [items[m] for m in ours(masks)], parts, kaug, ktr, vs, prev,
            *((raw_k, k_gain, F32) if final else (None, None, BF16)),
        )
        prev = (dk, dv)
        for m, x in zip(masks, dqs):
            if m & 1:
                met[m ^ 1] = swap(x, "frame", pair)
            elif m:
                both = (x.astype(F32) + met[m].astype(F32)).astype(BF16)
                dk, dv, both = lax.optimization_barrier((*prev, both))
                prev = (dk, dv)
                recvs.append(swap(both, "frame", m * pair))
    recvs.append(met[0])
    keep, kg, vg = dqs[0], dk, dv
    if pair == 2:
        join = lambda a, b: jnp.where(
            core[0] == 0, jnp.concatenate([a, b], axis=1), jnp.concatenate([b, a], axis=1)
        )
        kg = join(kg[0], swap(kg[1], "frame", 1))
        vg = join(vg[0], swap(vg[1], "frame", 1))
    else:
        kg, vg = kg[0], vg[0]
    columns = w_query.shape[0]
    hbits = bits_of(heads)
    flows = min(2, max(1, len(hbits)))
    own_cols = columns // heads
    cw = own_cols // flows
    bn = next(b for b in (1024, 512, 256, 128) if cw % b == 0)
    h = lax.axis_index("head").astype(jnp.int32)
    first, second = [], []
    turns = []
    for i in range(flows):
        turn = hbits[i:] + hbits[:i]
        turns.append(turn)
        masks = split_order(turn)
        cut = len(masks) // 2 if turn else 1
        for chosen, into in ((masks[:cut], second), (masks[cut:], first)):
            into += [(m, i * cw // bn + j) for m in chosen for j in range(cw // bn)]

    def text(entries, kind, after):
        where = (h ^ np.array([m for m, _ in entries], np.int32)) * (own_cols // bn)
        tab = jnp.concatenate([core, where + np.array([o for _, o in entries], np.int32)])
        return text_call(tab, keep, recvs, queries, got_q, q_gain, w_query, pair, bn, (kind, BF16), hd, after)

    whole_of = lambda y: y[0] if pair == 1 else y[0] + swap(y[1], "frame", 1).astype(F32)
    pieces = lambda y: [y[:, i * y.shape[1] // flows : (i + 1) * y.shape[1] // flows] for i in range(flows)]
    moved, sums = [], []
    if hbits:
        sums = [s.astype(BF16) for s in pieces(whole_of(text(first, F32, [])))]
        moved = [swap(s, "head", t[0]) for s, t in zip(sums, turns)]
    outs = []
    for i, both in enumerate(pieces(whole_of(text(second, F32, sums)))):
        if hbits:
            both = both + moved[i].astype(F32)
        for bit in turns[i][1:]:
            mid = both.shape[1] // 2
            both = both[:, :mid] + swap(both[:, mid:].astype(BF16), "head", bit).astype(F32)
        outs.append(both)
    return (jnp.concatenate(outs, axis=1), kg, vg)


def solution(mesh):
    return jax.shard_map(
        local,
        mesh=mesh,
        in_specs=(
            P("frame", "head"),
            P(),
            P("frame", "head"),
            P(),
            P("frame", "head"),
            P("frame", "head"),
            P(None, "head"),
            P(None, "frame"),
            P("frame"),
        ),
        out_specs=(P("frame", "head"), P("frame", "head"), P("frame", "head")),
        check_vma=False,
    )
```
